32 devices in a mesh: gx: 2 (over x), gy: 16 (over z, y, core).
Axes of the slice: x: 2, y: 2, z: 4, core: 2. Of those that a mesh axis runs over, the one named last changes fastest.
Arguments:
- trial: float32 [49152, 384], P(('gx', 'gy')), may hold values from -30 to 30
- resid: float32 [49152, 128], P(('gx', 'gy')), may hold values from -500 to 500
- energy: float32 [49152], P(('gx', 'gy')), may hold values from 1 to 10
- shift: float32 [128], replicated, may hold values from 0.05 to 0.5
Outputs:
- basis: float32 [49152, 128], P(('gx', 'gy'))
The draws below stay inside these ranges and needn't reach their ends.
All inputs are finite; a program needn't handle non-finite values.
Results may differ from the reference program's by a relative error of at most 0.0003.
Values sent between devices are 32-bit elements; how exact they have to be, the bound alone decides.
A program may use at most 64 MiB of HBM per device.

```python
import math
import jax
import jax.numpy as jnp
from jax import lax

KEEP = 384
NEW = 128
NPAIR = 49152


side_share = 0.01


def base_noise(key, label, height, breadth):
    subkey = jax.random.fold_in(jax.random.fold_in(key, 5101), label)
    return jax.random.truncated_normal(subkey, -5.0, 5.0, (height, breadth), jnp.float32)


def row_scale():
    place = jnp.arange(NPAIR, dtype=jnp.float32) / (NPAIR - 1)
    return jnp.exp(place * math.log(3.0))[:, None]


def energies(key):
    subkey = jax.random.fold_in(jax.random.fold_in(key, 5101), 11)
    level = jax.random.uniform(subkey, (NPAIR,), jnp.float32, 0.0, 1.0)
    return jnp.exp(level * math.log(9.99))


def shifts(key):
    subkey = jax.random.fold_in(jax.random.fold_in(key, 5101), 12)
    return jax.random.uniform(subkey, (NEW,), jnp.float32, 0.05, 0.5)


def draw_trial(key, part):
    return base_noise(key, 1, NPAIR, KEEP) * row_scale()


def draw_energy(key, part):
    return energies(key)


def draw_shift(key, part):
    return shifts(key)


def draw_resid(key, part):
    stored = base_noise(key, 1, NPAIR, KEEP)
    mixkey = jax.random.fold_in(jax.random.fold_in(key, 5101), 2)
    mixing = jax.random.truncated_normal(mixkey, -5.0, 5.0, (KEEP, NEW), jnp.float32) / math.sqrt(KEEP)
    owned = base_noise(key, 5, NPAIR, NEW)
    inside = jnp.dot(stored, mixing, precision=lax.Precision.HIGHEST, preferred_element_type=jnp.float32)
    target = jnp.clip(inside, -7.9, 7.9) + side_share * owned
    target = target * row_scale()
    return target * (energies(key)[:, None] - shifts(key)[None, :])


def setup_inputs(seed: int = 0) -> dict:
    key_list = jax.random.split(jax.random.key(seed), 5)
    return {
        "trial": draw_trial(jax.random.fold_in(key_list[4], 71), 0),
        "resid": draw_resid(jax.random.fold_in(key_list[4], 71), 0),
        "energy": draw_energy(jax.random.fold_in(key_list[4], 71), 0),
        "shift": draw_shift(jax.random.fold_in(key_list[4], 71), 0),
    }


def fdot(left, right):
    return jnp.dot(left.astype(jnp.float32), right.astype(jnp.float32), precision=lax.Precision.HIGHEST, preferred_element_type=jnp.float32)

def reference(trial, resid, energy, shift):
    count = trial.shape[0]
    work = resid / (energy[:, None] - shift[None, :])
    for sweep in range(2):
        coef = fdot(trial.T, work) / count
        work = work - fdot(trial, coef)
    gram = fdot(work.T, work) / count
    lower = jnp.linalg.cholesky(gram)
    return jax.scipy.linalg.solve_triangular(lower, work.T, lower=True).T
```

```python
import functools

import jax
import jax.numpy as jnp
from jax import lax
from jax.experimental import pallas as pl
from jax.experimental.pallas import tpu as pltpu
from jax.sharding import PartitionSpec as P

MESH = pl.DeviceIdType.MESH
LANES = 128


def dot(left, right, dims):
    return lax.dot_general(
        left, right, (dims, ((), ())),
        precision=lax.Precision.HIGHEST, preferred_element_type=jnp.float32,
    )


def chunk_rows(total, owners):
    rows = 8
    while total % rows or total // rows > owners:
        rows += 8
    return rows


def ranges(count, step):
    return [(start, min(step, count - start)) for start in range(0, count, step)]


def kernel(
    nx, ny, count, trial, resid, energy, shift, work, gram,
    part, swap, acc, landed, red, full, gpart, glanded, gred,
    swap_send, swap_recv, rs_send, rs_recv, ag_send, ag_recv, fw_send, fw_recv,
    gs_send, gs_recv, ga_send, ga_recv,
):
    ix, iy = lax.axis_index("gx"), lax.axis_index("gy")
    pairs_y = ny // 2
    np_ = nx * pairs_y
    ndev = nx * ny
    me, core = ix * pairs_y + iy // 2, iy % 2
    flat = me * 2 + core
    keep = trial.shape[1] // LANES
    rows = trial.shape[0]
    half = acc.shape[0]
    rs_rows = red.shape[0]
    owners = half // rs_rows
    g_rows = gred.shape[0]
    g_owners = LANES // g_rows

    def where(pair, which):
        return (pair // pairs_y, (pair % pairs_y) * 2 + which)

    def others(total, mine, body):
        def step(k, carry):
            body(lax.rem(mine + k, total))
            return carry
        lax.fori_loop(1, total, step, 0)

    barrier = pltpu.get_barrier_semaphore()

    def greet(other):
        pl.semaphore_signal(barrier, inc=1, device_id=where(other // 2, other % 2), device_id_type=MESH)
    others(ndev, flat, greet)

    for block in range(rows // LANES):
        span = pl.ds(block * LANES, LANES)
        level = jnp.broadcast_to(energy[block:block + 1, :], (LANES, LANES)).T
        work[span, :] = resid[span, :] / (level - shift[...])

    slots = {}
    place = 0
    for i in range(keep):
        slots["r", i] = place
        place += 1
    for i in range(keep):
        for j in range(i, keep):
            slots[i, j] = place
            place += 1
    for i in range(keep):
        left = pl.ds(i * LANES, LANES)
        first = None
        second = None
        for start, size in ranges(rows, 512):
            span = pl.ds(start, size)
            one = dot(trial[span, left], work[span, :], ((0,), (0,)))
            two = dot(trial[span, left], trial[span, i * LANES:], ((0,), (0,)))
            first = one if first is None else first + one
            second = two if second is None else second + two
        part[pl.ds(slots["r", i] * LANES, LANES), :] = first
        for j in range(i, keep):
            part[pl.ds(slots[i, j] * LANES, LANES), :] = second[:, (j - i) * LANES:(j - i + 1) * LANES]
    if place * LANES < 2 * half:
        part[pl.ds(place * LANES, 2 * half - place * LANES), :] = jnp.zeros(
            (2 * half - place * LANES, LANES), jnp.float32)

    pl.semaphore_wait(barrier, ndev - 1)

    def half_of(which):
        return pl.ds(pl.multiple_of(which * half, 8), half)

    def rows_of(index, size, base=0):
        return pl.ds(pl.multiple_of(base + index * size, 8), size)

    exchange = pltpu.make_async_remote_copy(
        src_ref=part.at[half_of(1 - core)], dst_ref=swap, send_sem=swap_send, recv_sem=swap_recv,
        device_id=where(me, 1 - core), device_id_type=MESH)
    exchange.start()
    exchange.wait()
    acc[...] = part[half_of(core), :] + swap[...]

    def scatter(other):
        return pltpu.make_async_remote_copy(
            src_ref=acc.at[rows_of(other, rs_rows)], dst_ref=landed.at[me],
            send_sem=rs_send.at[other], recv_sem=rs_recv.at[me],
            device_id=where(other, core), device_id_type=MESH)

    def scatter_in(other):
        return pltpu.make_async_remote_copy(
            src_ref=acc.at[rows_of(0, rs_rows)], dst_ref=landed.at[other],
            send_sem=rs_send.at[other], recv_sem=rs_recv.at[other],
            device_id=where(other, core), device_id_type=MESH)

    def guarded(limit, body):
        def run(other):
            if limit >= np_:
                body(other)
            else:
                @pl.when(other < limit)
                def _():
                    body(other)
        return run

    others(np_, me, guarded(owners, lambda other: scatter(other).start()))

    base = core * half

    def gather(other):
        return pltpu.make_async_remote_copy(
            src_ref=red, dst_ref=full.at[rows_of(me, rs_rows, base)],
            send_sem=ag_send.at[other], recv_sem=ag_recv.at[me],
            device_id=where(other, core), device_id_type=MESH)

    def gather_in(other):
        return pltpu.make_async_remote_copy(
            src_ref=red, dst_ref=full.at[rows_of(other, rs_rows, base)],
            send_sem=ag_send.at[other], recv_sem=ag_recv.at[other],
            device_id=where(other, core), device_id_type=MESH)

    def forward(owner, source):
        return pltpu.make_async_remote_copy(
            src_ref=source, dst_ref=full.at[rows_of(owner, rs_rows, base)],
            send_sem=fw_send.at[owner], recv_sem=fw_recv.at[owner],
            device_id=where(me, 1 - core), device_id_type=MESH)

    def forward_in(owner):
        return pltpu.make_async_remote_copy(
            src_ref=red, dst_ref=full.at[rows_of(owner, rs_rows, half - base)],
            send_sem=fw_send.at[owner], recv_sem=fw_recv.at[owner],
            device_id=where(me, 1 - core), device_id_type=MESH)

    @pl.when(me < owners)
    def _():
        others(np_, me, lambda other: scatter_in(other).wait_recv())
        landed[me] = acc[rows_of(me, rs_rows), :]
        red[...] = lax.fori_loop(0, np_, lambda k, total: total + landed[k], jnp.zeros(red.shape, jnp.float32))
        others(np_, me, lambda other: gather(other).start())
        forward(me, red).start()
        full[rows_of(me, rs_rows, base), :] = red[...]

    def relay(other):
        gather_in(other).wait_recv()
        forward(other, full.at[rows_of(other, rs_rows, base)]).start()
    others(np_, me, guarded(owners, relay))
    lax.fori_loop(0, owners, lambda k, carry: (forward_in(k).wait_recv(), carry)[1], 0)

    raw = [full[pl.ds(slots["r", i] * LANES, LANES), :] for i in range(keep)]
    first = [one / count for one in raw]
    total = []
    for i in range(keep):
        metric = None
        for j in range(keep):
            block = full[pl.ds(slots[min(i, j), max(i, j)] * LANES, LANES), :]
            term = dot(block, first[j], ((1,), (0,)) if i <= j else ((0,), (0,)))
            metric = term if metric is None else metric + term
        total.append(first[i] + (raw[i] - metric) / count)
    coef = jnp.concatenate(total, axis=0)
    square = None
    for start, size in ranges(rows, 512):
        span = pl.ds(start, size)
        block = work[span, :] - dot(trial[span, :], coef, ((1,), (0,)))
        work[span, :] = block
        term = dot(block, block, ((0,), (0,)))
        square = term if square is None else square + term
    gpart[...] = square

    def gscatter(other):
        return pltpu.make_async_remote_copy(
            src_ref=gpart.at[rows_of(other, g_rows)], dst_ref=glanded.at[flat],
            send_sem=gs_send.at[other], recv_sem=gs_recv.at[flat],
            device_id=where(other, 0), device_id_type=MESH)

    def gscatter_in(other):
        return pltpu.make_async_remote_copy(
            src_ref=gpart.at[rows_of(0, g_rows)], dst_ref=glanded.at[other],
            send_sem=gs_send.at[0], recv_sem=gs_recv.at[other],
            device_id=where(other // 2, other % 2), device_id_type=MESH)

    def ggather(other):
        return pltpu.make_async_remote_copy(
            src_ref=gred, dst_ref=gram.at[rows_of(me, g_rows)],
            send_sem=ga_send.at[other], recv_sem=ga_recv.at[me],
            device_id=where(other // 2, other % 2), device_id_type=MESH)

    def ggather_in(owner):
        return pltpu.make_async_remote_copy(
            src_ref=gred, dst_ref=gram.at[rows_of(owner, g_rows)],
            send_sem=ga_send.at[0], recv_sem=ga_recv.at[owner],
            device_id=where(owner, 0), device_id_type=MESH)

    others(np_, me, guarded(g_owners, lambda other: gscatter(other).start()))

    @pl.when(jnp.logical_and(core == 1, me < g_owners))
    def _():
        gscatter(me).start()

    @pl.when(jnp.logical_and(core == 0, me < g_owners))
    def _():
        others(ndev, flat, lambda other: gscatter_in(other).wait_recv())
        glanded[flat] = gpart[rows_of(me, g_rows), :]
        gred[...] = lax.fori_loop(
            0, ndev, lambda k, total: total + glanded[k], jnp.zeros(gred.shape, jnp.float32)) / count
        others(ndev, flat, lambda other: ggather(other).start())
        gram[rows_of(me, g_rows), :] = gred[...]

    others(np_, me, guarded(g_owners, lambda other: ggather_in(other).wait_recv()))

    @pl.when(jnp.logical_and(core == 1, me < g_owners))
    def _():
        ggather_in(me).wait_recv()

    others(np_, me, guarded(owners, lambda other: scatter(other).wait_send()))

    @pl.when(me < owners)
    def _():
        others(np_, me, lambda other: gather(other).wait_send())
    lax.fori_loop(0, owners, lambda k, carry: (forward_in(k).wait_send(), carry)[1], 0)
    others(np_, me, guarded(g_owners, lambda other: gscatter(other).wait_send()))

    @pl.when(jnp.logical_and(core == 1, me < g_owners))
    def _():
        gscatter(me).wait_send()

    @pl.when(jnp.logical_and(core == 0, me < g_owners))
    def _():
        others(ndev, flat, lambda other: ggather(other).wait_send())


def normalize(block, gram):
    lower = jnp.linalg.cholesky(gram)
    return jax.scipy.linalg.solve_triangular(lower, block.T, lower=True).T


def per_device(nx, ny, trial, resid, energy, shift):
    rows, kept = trial.shape
    new = resid.shape[1]
    keep = kept // LANES
    blocks = keep + keep * (keep + 1) // 2
    half = (blocks + 1) // 2 * LANES
    np_ = nx * (ny // 2)
    rs_rows = chunk_rows(half, np_)
    owners = half // rs_rows
    g_rows = chunk_rows(LANES, np_)
    f32 = jnp.float32
    dma = pltpu.SemaphoreType.DMA
    vmem = pl.BlockSpec(memory_space=pltpu.VMEM)
    work, gram = pl.pallas_call(
        functools.partial(kernel, nx, ny, float(rows * nx * ny)),
        name="project",
        out_shape=(jax.ShapeDtypeStruct((rows, new), f32), jax.ShapeDtypeStruct((new, new), f32)),
        in_specs=[vmem] * 4,
        out_specs=(vmem, vmem),
        scratch_shapes=[
            pltpu.VMEM((2 * half, LANES), f32),
            pltpu.VMEM((half, LANES), f32),
            pltpu.VMEM((half, LANES), f32),
            pltpu.VMEM((np_, rs_rows, LANES), f32),
            pltpu.VMEM((rs_rows, LANES), f32),
            pltpu.VMEM((2 * half, LANES), f32),
            pltpu.VMEM((LANES, LANES), f32),
            pltpu.VMEM((nx * ny, g_rows, LANES), f32),
            pltpu.VMEM((g_rows, LANES), f32),
            dma, dma, dma((np_,)), dma((np_,)), dma((np_,)), dma((np_,)), dma((owners,)), dma((owners,)),
            dma((np_,)), dma((nx * ny,)), dma((nx * ny,)), dma((np_,)),
        ],
        compiler_params=pltpu.CompilerParams(collective_id=0, has_side_effects=True),
    )(trial, resid, energy.reshape(rows // LANES, LANES), shift.reshape(1, new))
    return normalize(work, gram)


def solution(mesh):
    in_specs = (P(("gx", "gy"), None), P(("gx", "gy"), None), P(("gx", "gy")), P())
    out_specs = P(("gx", "gy"), None)
    body = functools.partial(per_device, mesh.shape["gx"], mesh.shape["gy"])
    return jax.shard_map(body, mesh=mesh, in_specs=in_specs, out_specs=out_specs, check_vma=False)
```

```python
import functools

import jax
import jax.numpy as jnp
from jax import lax
from jax.experimental import pallas as pl
from jax.experimental.pallas import tpu as pltpu
from jax.sharding import PartitionSpec as P

MESH = pl.DeviceIdType.MESH
LANES = 128


def dot(left, right, dims):
    return lax.dot_general(
        left, right, (dims, ((), ())),
        precision=lax.Precision.HIGHEST, preferred_element_type=jnp.float32,
    )


def chunk_rows(total, owners):
    rows = 8
    while total % rows or total // rows > owners:
        rows += 8
    return rows


def ranges(count, step):
    return [(start, min(step, count - start)) for start in range(0, count, step)]


def split(values):
    high = values.astype(jnp.bfloat16)
    rest = values - high.astype(jnp.float32)
    middle = rest.astype(jnp.bfloat16)
    low = (rest - middle.astype(jnp.float32)).astype(jnp.bfloat16)
    return high, middle, low


def outer(left, right):
    a, b, c = split(left)
    d, e, f = split(right)
    return lax.dot_general(
        jnp.concatenate([a, a, b, b, a, c], 0), jnp.concatenate([d, e, d, e, f, d], 0),
        (((0,), (0,)), ((), ())), preferred_element_type=jnp.float32)


def inverse_factor(square, width):
    size = square.shape[0]
    row = lax.broadcasted_iota(jnp.int32, (size, size), 0)
    col = lax.broadcasted_iota(jnp.int32, (size, size), 1)
    both = jnp.concatenate([square, (row == col).astype(jnp.float32)], axis=1)
    local = lax.broadcasted_iota(jnp.int32, (width, size), 0)
    out = []
    for start in range(0, size, width):
        slab, side = both[:width, :size], both[:width, size:]
        cols = [jnp.broadcast_to(slab[:, start + j:start + j + 1], (width, size)) for j in range(width)]
        scale = jnp.ones((width, size), jnp.float32)
        for j in range(width):
            inverse = 1.0 / cols[j][j:j + 1, :]
            factor = jnp.where(local > j, cols[j] * inverse, 0.0)
            scale = jnp.where(local == j, inverse, scale)
            for m in range(j + 1, width):
                cols[m] = cols[m] - factor * cols[m][j:j + 1, :]
            slab = slab - factor * slab[j:j + 1, :]
            side = side - factor * side[j:j + 1, :]
        out.append(side * jnp.sqrt(scale))
        if start + width < size:
            update = outer(slab * scale, jnp.concatenate([slab, side], axis=1))
            both = both[width:] - update[start + width:]
    return jnp.concatenate(out, axis=0)


def kernel(
    nx, ny, count, trial, resid, energy, shift, basis,
    work, gram, part, swap, acc, landed, red, full, gpart, glanded, gred,
    swap_send, swap_recv, rs_send, rs_recv, ag_send, ag_recv, fw_send, fw_recv,
    gs_send, gs_recv, ga_send, ga_recv,
):
    ix, iy = lax.axis_index("gx"), lax.axis_index("gy")
    pairs_y = ny // 2
    np_ = nx * pairs_y
    ndev = nx * ny
    me, core = ix * pairs_y + iy // 2, iy % 2
    flat = me * 2 + core
    keep = trial.shape[1] // LANES
    rows = trial.shape[0]
    half = acc.shape[0]
    rs_rows = red.shape[0]
    owners = half // rs_rows
    g_rows = gred.shape[0]
    g_owners = LANES // g_rows

    def where(pair, which):
        return (pair // pairs_y, (pair % pairs_y) * 2 + which)

    def others(total, mine, body):
        def step(k, carry):
            body(lax.rem(mine + k, total))
            return carry
        lax.fori_loop(1, total, step, 0)

    barrier = pltpu.get_barrier_semaphore()

    def greet(other):
        pl.semaphore_signal(barrier, inc=1, device_id=where(other // 2, other % 2), device_id_type=MESH)
    others(ndev, flat, greet)

    for block in range(rows // LANES):
        span = pl.ds(block * LANES, LANES)
        level = jnp.broadcast_to(energy[block:block + 1, :], (LANES, LANES)).T
        work[span, :] = resid[span, :] / (level - shift[...])

    slots = {}
    place = 0
    for i in range(keep):
        slots["r", i] = place
        place += 1
    for i in range(keep):
        for j in range(i, keep):
            slots[i, j] = place
            place += 1
    for i in range(keep):
        left = pl.ds(i * LANES, LANES)
        first = None
        second = None
        for start, size in ranges(rows, 512):
            span = pl.ds(start, size)
            one = dot(trial[span, left], work[span, :], ((0,), (0,)))
            two = dot(trial[span, left], trial[span, i * LANES:], ((0,), (0,)))
            first = one if first is None else first + one
            second = two if second is None else second + two
        part[pl.ds(slots["r", i] * LANES, LANES), :] = first
        for j in range(i, keep):
            part[pl.ds(slots[i, j] * LANES, LANES), :] = second[:, (j - i) * LANES:(j - i + 1) * LANES]
    if place * LANES < 2 * half:
        part[pl.ds(place * LANES, 2 * half - place * LANES), :] = jnp.zeros(
            (2 * half - place * LANES, LANES), jnp.float32)

    pl.semaphore_wait(barrier, ndev - 1)

    def half_of(which):
        return pl.ds(pl.multiple_of(which * half, 8), half)

    def rows_of(index, size, base=0):
        return pl.ds(pl.multiple_of(base + index * size, 8), size)

    exchange = pltpu.make_async_remote_copy(
        src_ref=part.at[half_of(1 - core)], dst_ref=swap, send_sem=swap_send, recv_sem=swap_recv,
        device_id=where(me, 1 - core), device_id_type=MESH)
    exchange.start()
    exchange.wait()
    acc[...] = part[half_of(core), :] + swap[...]

    def scatter(other):
        return pltpu.make_async_remote_copy(
            src_ref=acc.at[rows_of(other, rs_rows)], dst_ref=landed.at[me],
            send_sem=rs_send.at[other], recv_sem=rs_recv.at[me],
            device_id=where(other, core), device_id_type=MESH)

    def scatter_in(other):
        return pltpu.make_async_remote_copy(
            src_ref=acc.at[rows_of(0, rs_rows)], dst_ref=landed.at[other],
            send_sem=rs_send.at[other], recv_sem=rs_recv.at[other],
            device_id=where(other, core), device_id_type=MESH)

    def guarded(limit, body):
        def run(other):
            if limit >= np_:
                body(other)
            else:
                @pl.when(other < limit)
                def _():
                    body(other)
        return run

    others(np_, me, guarded(owners, lambda other: scatter(other).start()))

    base = core * half

    def gather(other):
        return pltpu.make_async_remote_copy(
            src_ref=red, dst_ref=full.at[rows_of(me, rs_rows, base)],
            send_sem=ag_send.at[other], recv_sem=ag_recv.at[me],
            device_id=where(other, core), device_id_type=MESH)

    def gather_in(other):
        return pltpu.make_async_remote_copy(
            src_ref=red, dst_ref=full.at[rows_of(other, rs_rows, base)],
            send_sem=ag_send.at[other], recv_sem=ag_recv.at[other],
            device_id=where(other, core), device_id_type=MESH)

    def forward(owner, source):
        return pltpu.make_async_remote_copy(
            src_ref=source, dst_ref=full.at[rows_of(owner, rs_rows, base)],
            send_sem=fw_send.at[owner], recv_sem=fw_recv.at[owner],
            device_id=where(me, 1 - core), device_id_type=MESH)

    def forward_in(owner):
        return pltpu.make_async_remote_copy(
            src_ref=red, dst_ref=full.at[rows_of(owner, rs_rows, half - base)],
            send_sem=fw_send.at[owner], recv_sem=fw_recv.at[owner],
            device_id=where(me, 1 - core), device_id_type=MESH)

    @pl.when(me < owners)
    def _():
        others(np_, me, lambda other: scatter_in(other).wait_recv())
        landed[me] = acc[rows_of(me, rs_rows), :]
        red[...] = lax.fori_loop(0, np_, lambda k, total: total + landed[k], jnp.zeros(red.shape, jnp.float32))
        others(np_, me, lambda other: gather(other).start())
        forward(me, red).start()
        full[rows_of(me, rs_rows, base), :] = red[...]

    def relay(other):
        gather_in(other).wait_recv()
        forward(other, full.at[rows_of(other, rs_rows, base)]).start()
    others(np_, me, guarded(owners, relay))
    lax.fori_loop(0, owners, lambda k, carry: (forward_in(k).wait_recv(), carry)[1], 0)

    raw = [full[pl.ds(slots["r", i] * LANES, LANES), :] for i in range(keep)]
    first = [one / count for one in raw]
    total = []
    for i in range(keep):
        metric = None
        for j in range(keep):
            block = full[pl.ds(slots[min(i, j), max(i, j)] * LANES, LANES), :]
            term = dot(block, first[j], ((1,), (0,)) if i <= j else ((0,), (0,)))
            metric = term if metric is None else metric + term
        total.append(first[i] + (raw[i] - metric) / count)
    coef = jnp.concatenate(total, axis=0)
    square = None
    for start, size in ranges(rows, 512):
        span = pl.ds(start, size)
        block = work[span, :] - dot(trial[span, :], coef, ((1,), (0,)))
        work[span, :] = block
        term = dot(block, block, ((0,), (0,)))
        square = term if square is None else square + term
    gpart[...] = square

    def gscatter(other):
        return pltpu.make_async_remote_copy(
            src_ref=gpart.at[rows_of(other, g_rows)], dst_ref=glanded.at[flat],
            send_sem=gs_send.at[other], recv_sem=gs_recv.at[flat],
            device_id=where(other, 0), device_id_type=MESH)

    def gscatter_in(other):
        return pltpu.make_async_remote_copy(
            src_ref=gpart.at[rows_of(0, g_rows)], dst_ref=glanded.at[other],
            send_sem=gs_send.at[0], recv_sem=gs_recv.at[other],
            device_id=where(other // 2, other % 2), device_id_type=MESH)

    def ggather(other):
        return pltpu.make_async_remote_copy(
            src_ref=gred, dst_ref=gram.at[rows_of(me, g_rows)],
            send_sem=ga_send.at[other], recv_sem=ga_recv.at[me],
            device_id=where(other // 2, other % 2), device_id_type=MESH)

    def ggather_in(owner):
        return pltpu.make_async_remote_copy(
            src_ref=gred, dst_ref=gram.at[rows_of(owner, g_rows)],
            send_sem=ga_send.at[0], recv_sem=ga_recv.at[owner],
            device_id=where(owner, 0), device_id_type=MESH)

    others(np_, me, guarded(g_owners, lambda other: gscatter(other).start()))

    @pl.when(jnp.logical_and(core == 1, me < g_owners))
    def _():
        gscatter(me).start()

    @pl.when(jnp.logical_and(core == 0, me < g_owners))
    def _():
        others(ndev, flat, lambda other: gscatter_in(other).wait_recv())
        glanded[flat] = gpart[rows_of(me, g_rows), :]
        gred[...] = lax.fori_loop(
            0, ndev, lambda k, total: total + glanded[k], jnp.zeros(gred.shape, jnp.float32)) / count
        others(ndev, flat, lambda other: ggather(other).start())
        gram[rows_of(me, g_rows), :] = gred[...]

    others(np_, me, guarded(g_owners, lambda other: ggather_in(other).wait_recv()))

    @pl.when(jnp.logical_and(core == 1, me < g_owners))
    def _():
        ggather_in(me).wait_recv()

    inverse = inverse_factor(gram[...], 16)
    for start, size in ranges(rows, 512):
        span = pl.ds(start, size)
        basis[span, :] = dot(work[span, :], inverse, ((1,), (1,)))

    others(np_, me, guarded(owners, lambda other: scatter(other).wait_send()))

    @pl.when(me < owners)
    def _():
        others(np_, me, lambda other: gather(other).wait_send())
    lax.fori_loop(0, owners, lambda k, carry: (forward_in(k).wait_send(), carry)[1], 0)
    others(np_, me, guarded(g_owners, lambda other: gscatter(other).wait_send()))

    @pl.when(jnp.logical_and(core == 1, me < g_owners))
    def _():
        gscatter(me).wait_send()

    @pl.when(jnp.logical_and(core == 0, me < g_owners))
    def _():
        others(ndev, flat, lambda other: ggather(other).wait_send())


def per_device(nx, ny, trial, resid, energy, shift):
    rows, kept = trial.shape
    new = resid.shape[1]
    keep = kept // LANES
    blocks = keep + keep * (keep + 1) // 2
    half = (blocks + 1) // 2 * LANES
    np_ = nx * (ny // 2)
    rs_rows = chunk_rows(half, np_)
    owners = half // rs_rows
    g_rows = chunk_rows(LANES, np_)
    f32 = jnp.float32
    dma = pltpu.SemaphoreType.DMA
    vmem = pl.BlockSpec(memory_space=pltpu.VMEM)
    return pl.pallas_call(
        functools.partial(kernel, nx, ny, float(rows * nx * ny)),
        name="project",
        out_shape=jax.ShapeDtypeStruct((rows, new), f32),
        in_specs=[vmem] * 4,
        out_specs=vmem,
        scratch_shapes=[
            pltpu.VMEM((rows, new), f32),
            pltpu.VMEM((new, new), f32),
            pltpu.VMEM((2 * half, LANES), f32),
            pltpu.VMEM((half, LANES), f32),
            pltpu.VMEM((half, LANES), f32),
            pltpu.VMEM((np_, rs_rows, LANES), f32),
            pltpu.VMEM((rs_rows, LANES), f32),
            pltpu.VMEM((2 * half, LANES), f32),
            pltpu.VMEM((LANES, LANES), f32),
            pltpu.VMEM((nx * ny, g_rows, LANES), f32),
            pltpu.VMEM((g_rows, LANES), f32),
            dma, dma, dma((np_,)), dma((np_,)), dma((np_,)), dma((np_,)), dma((owners,)), dma((owners,)),
            dma((np_,)), dma((nx * ny,)), dma((nx * ny,)), dma((np_,)),
        ],
        compiler_params=pltpu.CompilerParams(collective_id=0, has_side_effects=True),
    )(trial, resid, energy.reshape(rows // LANES, LANES), shift.reshape(1, new))


def solution(mesh):
    in_specs = (P(("gx", "gy"), None), P(("gx", "gy"), None), P(("gx", "gy")), P())
    out_specs = P(("gx", "gy"), None)
    body = functools.partial(per_device, mesh.shape["gx"], mesh.shape["gy"])
    return jax.shard_map(body, mesh=mesh, in_specs=in_specs, out_specs=out_specs, check_vma=False)
```

```python
import functools

import jax
import jax.numpy as jnp
from jax import lax
from jax.experimental import pallas as pl
from jax.experimental.pallas import tpu as pltpu
from jax.sharding import PartitionSpec as P

MESH = pl.DeviceIdType.MESH
LANES = 128
HALF = LANES // 2


def bdot(left, right, dims):
    return lax.dot_general(left, right, (dims, ((), ())), preferred_element_type=jnp.float32)


def chunk_rows(total, owners):
    return -(-total // (8 * owners)) * 8


def ranges(count, step):
    return [(start, min(step, count - start)) for start in range(0, count, step)]


def split(values):
    high = values.astype(jnp.bfloat16)
    rest = values - high.astype(jnp.float32)
    middle = rest.astype(jnp.bfloat16)
    low = (rest - middle.astype(jnp.float32)).astype(jnp.bfloat16)
    return high, middle, low


def dot(left, right, dims):
    return lax.dot_general(
        left, right, (dims, ((), ())),
        precision=lax.Precision.HIGHEST, preferred_element_type=jnp.float32,
    )


def wide(high, middle, low, right):
    a, b, c = split(right)
    both = jnp.concatenate([a, b], axis=1)
    width = right.shape[1]
    one = bdot(high, both, ((1,), (0,)))
    two = bdot(middle, both, ((1,), (0,)))
    rest = bdot(high, c, ((1,), (0,))) + bdot(low, a, ((1,), (0,)))
    return one[:, :width] + (one[:, width:] + two[:, :width] + (rest + two[:, width:]))


def outer(left, right):
    a, b, c = split(left)
    d, e, f = split(right)
    return lax.dot_general(
        jnp.concatenate([a, a, b, b, a, c], 0), jnp.concatenate([d, e, d, e, f, d], 0),
        (((0,), (0,)), ((), ())), preferred_element_type=jnp.float32)


def inverse_factor(square, width):
    size = square.shape[0]
    row = lax.broadcasted_iota(jnp.int32, (size, size), 0)
    col = lax.broadcasted_iota(jnp.int32, (size, size), 1)
    both = jnp.concatenate([square, (row == col).astype(jnp.float32)], axis=1)
    local = lax.broadcasted_iota(jnp.int32, (width, size), 0)
    out = []
    for start in range(0, size, width):
        slab, side = both[:width, :size], both[:width, size:]
        cols = [jnp.broadcast_to(slab[:, start + j:start + j + 1], (width, size)) for j in range(width)]
        scale = jnp.ones((width, size), jnp.float32)
        for j in range(width):
            inverse = 1.0 / cols[j][j:j + 1, :]
            factor = jnp.where(local > j, cols[j] * inverse, 0.0)
            scale = jnp.where(local == j, inverse, scale)
            for m in range(j + 1, width):
                cols[m] = cols[m] - factor * cols[m][j:j + 1, :]
            slab = slab - factor * slab[j:j + 1, :]
            side = side - factor * side[j:j + 1, :]
        out.append(side * jnp.sqrt(scale))
        if start + width < size:
            update = outer(slab * scale, jnp.concatenate([slab, side], axis=1))
            both = both[width:] - update[start + width:]
    return jnp.concatenate(out, axis=0)


def kernel(
    nx, ny, count, trial, resid, energy, shift, basis,
    xs, xh, xm, xl, wh, wm, wl, load, gram, part, swap, acc, landed, red, full, gpart, glanded, gred,
    swap_send, swap_recv, rs_send, rs_recv, ag_send, ag_recv, fw_send, fw_recv,
    gs_send, gs_recv, ga_send, ga_recv,
):
    ix, iy = lax.axis_index("gx"), lax.axis_index("gy")
    pairs_y = ny // 2
    np_ = nx * pairs_y
    ndev = nx * ny
    me, core = ix * pairs_y + iy // 2, iy % 2
    flat = me * 2 + core
    kept = trial.shape[1]
    keep = kept // LANES
    fetch = pltpu.make_async_copy(trial, xs.at[:, pl.ds(0, kept)], load)
    fetch.start()
    rows = trial.shape[0]
    half = acc.shape[0]
    rs_rows = red.shape[0]
    owners = half // rs_rows
    g_rows = gred.shape[0]
    g_owners = LANES // g_rows

    def where(pair, which):
        return (pair // pairs_y, (pair % pairs_y) * 2 + which)

    def others(total, mine, body):
        def step(k, carry):
            body(lax.rem(mine + k, total))
            return carry
        lax.fori_loop(1, total, step, 0)

    barrier = pltpu.get_barrier_semaphore()

    def greet(other):
        pl.semaphore_signal(barrier, inc=1, device_id=where(other // 2, other % 2), device_id_type=MESH)
    others(ndev, flat, greet)

    for block in range(rows // LANES):
        span = pl.ds(block * LANES, LANES)
        level = jnp.broadcast_to(energy[block:block + 1, :], (LANES, LANES)).T
        xs[span, kept:] = resid[span, :] / (level - shift[...])
    fetch.wait()
    for start, size in ranges(rows, LANES):
        span = pl.ds(start, size)
        xh[span, :], xm[span, :], xl[span, :] = split(xs[span, :])

    slots = {}
    spans = []
    for i in range(keep):
        first_place = len(slots)
        for j in range(i, keep):
            slots[i, j] = len(slots)
        slots["r", i] = len(slots)
        spans.append((first_place * HALF, len(slots) * HALF))

    def stripe(i):
        left, right = pl.ds(i * LANES, LANES), slice(i * LANES, None)
        total = None
        for one, two in ((xm, xm), (xl, xh), (xh, xl), (xm, xh), (xh, xm), (xh, xh)):
            term = bdot(one[:, left], two[:, right], ((0,), (0,)))
            total = term if total is None else total + term
        for j in range(keep - i + 1):
            start = spans[i][0] + j * HALF
            for which in range(2):
                part[pl.ds(which * half + start, HALF), :] = total[
                    which * HALF:(which + 1) * HALF, j * LANES:(j + 1) * LANES]

    def read(name):
        return jnp.concatenate(
            [full[pl.ds(which * half + slots[name] * HALF, HALF), :] for which in range(2)], axis=0)

    def rows_of(index, size, base=0):
        return pl.ds(pl.multiple_of(base + index * size, 8), size)

    def exchange(i):
        low, high = spans[i]
        return pltpu.make_async_remote_copy(
            src_ref=part.at[pl.ds(pl.multiple_of((1 - core) * half + low, 8), high - low)],
            dst_ref=swap.at[pl.ds(low, high - low)],
            send_sem=swap_send.at[i], recv_sem=swap_recv.at[i],
            device_id=where(me, 1 - core), device_id_type=MESH)

    def scatter(other):
        return pltpu.make_async_remote_copy(
            src_ref=acc.at[rows_of(other, rs_rows)], dst_ref=landed.at[me],
            send_sem=rs_send.at[other], recv_sem=rs_recv.at[me],
            device_id=where(other, core), device_id_type=MESH)

    def scatter_in(other):
        return pltpu.make_async_remote_copy(
            src_ref=acc.at[rows_of(0, rs_rows)], dst_ref=landed.at[other],
            send_sem=rs_send.at[other], recv_sem=rs_recv.at[other],
            device_id=where(other, core), device_id_type=MESH)

    def guarded(limit, body):
        def run(other):
            if limit >= np_:
                body(other)
            else:
                @pl.when(other < limit)
                def _():
                    body(other)
        return run

    sent = [0]

    def absorb(i):
        low, high = spans[i]
        exchange(i).wait_recv()
        acc[pl.ds(low, high - low), :] = (
            part[pl.ds(pl.multiple_of(core * half + low, 8), high - low), :] + swap[pl.ds(low, high - low), :])
        begin, end = sent[0], owners if i == keep - 1 else high // rs_rows
        sent[0] = end

        def send(other):
            @pl.when(jnp.logical_and(other >= begin, other < end))
            def _():
                scatter(other).start()
        others(np_, me, send)

    if spans[-1][1] < half:
        acc[pl.ds(spans[-1][1], half - spans[-1][1]), :] = jnp.zeros((half - spans[-1][1], LANES), jnp.float32)
    for i in range(keep):
        stripe(i)
        if i == 0:
            pl.semaphore_wait(barrier, ndev - 1)
        exchange(i).start()
        if i > 0:
            absorb(i - 1)
    absorb(keep - 1)

    base = core * half

    def gather(other):
        return pltpu.make_async_remote_copy(
            src_ref=red, dst_ref=full.at[rows_of(me, rs_rows, base)],
            send_sem=ag_send.at[other], recv_sem=ag_recv.at[me],
            device_id=where(other, core), device_id_type=MESH)

    def gather_in(other):
        return pltpu.make_async_remote_copy(
            src_ref=red, dst_ref=full.at[rows_of(other, rs_rows, base)],
            send_sem=ag_send.at[other], recv_sem=ag_recv.at[other],
            device_id=where(other, core), device_id_type=MESH)

    def forward(owner, source):
        return pltpu.make_async_remote_copy(
            src_ref=source, dst_ref=full.at[rows_of(owner, rs_rows, base)],
            send_sem=fw_send.at[owner], recv_sem=fw_recv.at[owner],
            device_id=where(me, 1 - core), device_id_type=MESH)

    def forward_in(owner):
        return pltpu.make_async_remote_copy(
            src_ref=red, dst_ref=full.at[rows_of(owner, rs_rows, half - base)],
            send_sem=fw_send.at[owner], recv_sem=fw_recv.at[owner],
            device_id=where(me, 1 - core), device_id_type=MESH)

    @pl.when(me < owners)
    def _():
        others(np_, me, lambda other: scatter_in(other).wait_recv())
        landed[me] = acc[rows_of(me, rs_rows), :]
        red[...] = lax.fori_loop(0, np_, lambda k, total: total + landed[k], jnp.zeros(red.shape, jnp.float32))
        others(np_, me, lambda other: gather(other).start())
        forward(me, red).start()
        full[rows_of(me, rs_rows, base), :] = red[...]

    def relay(other):
        gather_in(other).wait_recv()
        forward(other, full.at[rows_of(other, rs_rows, base)]).start()
    others(np_, me, guarded(owners, relay))
    lax.fori_loop(0, owners, lambda k, carry: (forward_in(k).wait_recv(), carry)[1], 0)

    raw = [read(("r", i)) for i in range(keep)]
    first = [one / count for one in raw]
    total = []
    for i in range(keep):
        metric = None
        for j in range(keep):
            block = read((min(i, j), max(i, j)))
            term = dot(block, first[j], ((1,), (0,)) if i <= j else ((0,), (0,)))
            metric = term if metric is None else metric + term
        total.append(first[i] + (raw[i] - metric) / count)
    coef = jnp.concatenate(total, axis=0)
    for start, size in ranges(rows, 256):
        span = pl.ds(start, size)
        block = xs[span, kept:] - wide(xh[span, :kept], xm[span, :kept], xl[span, :kept], coef)
        wh[span, :], wm[span, :], wl[span, :] = split(block)
    ours = wh[...]
    high = bdot(ours, ours, ((0,), (0,)))
    cross = bdot(ours, wm[...], ((0,), (0,))) + bdot(ours, wl[...], ((0,), (0,)))
    gpart[...] = high + (cross + cross.T + bdot(wm[...], wm[...], ((0,), (0,))))

    def gscatter(other):
        return pltpu.make_async_remote_copy(
            src_ref=gpart.at[rows_of(other, g_rows)], dst_ref=glanded.at[flat],
            send_sem=gs_send.at[other], recv_sem=gs_recv.at[flat],
            device_id=where(other, 0), device_id_type=MESH)

    def gscatter_in(other):
        return pltpu.make_async_remote_copy(
            src_ref=gpart.at[rows_of(0, g_rows)], dst_ref=glanded.at[other],
            send_sem=gs_send.at[0], recv_sem=gs_recv.at[other],
            device_id=where(other // 2, other % 2), device_id_type=MESH)

    def ggather(other):
        return pltpu.make_async_remote_copy(
            src_ref=gred, dst_ref=gram.at[rows_of(me, g_rows)],
            send_sem=ga_send.at[other], recv_sem=ga_recv.at[me],
            device_id=where(other // 2, other % 2), device_id_type=MESH)

    def ggather_in(owner):
        return pltpu.make_async_remote_copy(
            src_ref=gred, dst_ref=gram.at[rows_of(owner, g_rows)],
            send_sem=ga_send.at[0], recv_sem=ga_recv.at[owner],
            device_id=where(owner, 0), device_id_type=MESH)

    others(np_, me, guarded(g_owners, lambda other: gscatter(other).start()))

    @pl.when(jnp.logical_and(core == 1, me < g_owners))
    def _():
        gscatter(me).start()

    @pl.when(jnp.logical_and(core == 0, me < g_owners))
    def _():
        others(ndev, flat, lambda other: gscatter_in(other).wait_recv())
        glanded[flat] = gpart[rows_of(me, g_rows), :]
        gred[...] = lax.fori_loop(
            0, ndev, lambda k, total: total + glanded[k], jnp.zeros(gred.shape, jnp.float32)) / count
        others(ndev, flat, lambda other: ggather(other).start())
        gram[rows_of(me, g_rows), :] = gred[...]

    others(np_, me, guarded(g_owners, lambda other: ggather_in(other).wait_recv()))

    @pl.when(jnp.logical_and(core == 1, me < g_owners))
    def _():
        ggather_in(me).wait_recv()

    inverse = inverse_factor(gram[...], 16).T
    for start, size in ranges(rows, 256):
        span = pl.ds(start, size)
        basis[span, :] = wide(wh[span, :], wm[span, :], wl[span, :], inverse)

    for i in range(keep):
        exchange(i).wait_send()
    others(np_, me, guarded(owners, lambda other: scatter(other).wait_send()))

    @pl.when(me < owners)
    def _():
        others(np_, me, lambda other: gather(other).wait_send())
    lax.fori_loop(0, owners, lambda k, carry: (forward_in(k).wait_send(), carry)[1], 0)
    others(np_, me, guarded(g_owners, lambda other: gscatter(other).wait_send()))

    @pl.when(jnp.logical_and(core == 1, me < g_owners))
    def _():
        gscatter(me).wait_send()

    @pl.when(jnp.logical_and(core == 0, me < g_owners))
    def _():
        others(ndev, flat, lambda other: ggather(other).wait_send())


def per_device(nx, ny, trial, resid, energy, shift):
    rows, kept = trial.shape
    new = resid.shape[1]
    keep = kept // LANES
    blocks = keep + keep * (keep + 1) // 2
    np_ = nx * (ny // 2)
    rs_rows = chunk_rows(blocks * HALF, np_)
    owners = -(-blocks * HALF // rs_rows)
    half = owners * rs_rows
    g_rows = chunk_rows(LANES, np_)
    f32 = jnp.float32
    dma = pltpu.SemaphoreType.DMA
    vmem = pl.BlockSpec(memory_space=pltpu.VMEM)
    return pl.pallas_call(
        functools.partial(kernel, nx, ny, float(rows * nx * ny)),
        name="project",
        out_shape=jax.ShapeDtypeStruct((rows, new), f32),
        in_specs=[pl.BlockSpec(memory_space=pl.ANY)] + [vmem] * 3,
        out_specs=vmem,
        scratch_shapes=[
            pltpu.VMEM((rows, kept + new), f32),
            *[pltpu.VMEM((rows, kept + new), jnp.bfloat16)] * 3,
            *[pltpu.VMEM((rows, new), jnp.bfloat16)] * 3,
            dma,
            pltpu.VMEM((new, new), f32),
            pltpu.VMEM((2 * half, LANES), f32),
            pltpu.VMEM((half, LANES), f32),
            pltpu.VMEM((half, LANES), f32),
            pltpu.VMEM((np_, rs_rows, LANES), f32),
            pltpu.VMEM((rs_rows, LANES), f32),
            pltpu.VMEM((2 * half, LANES), f32),
            pltpu.VMEM((LANES, LANES), f32),
            pltpu.VMEM((nx * ny, g_rows, LANES), f32),
            pltpu.VMEM((g_rows, LANES), f32),
            dma((keep,)), dma((keep,)), dma((np_,)), dma((np_,)), dma((np_,)), dma((np_,)), dma((owners,)), dma((owners,)),
            dma((np_,)), dma((nx * ny,)), dma((nx * ny,)), dma((np_,)),
        ],
        compiler_params=pltpu.CompilerParams(collective_id=0, has_side_effects=True),
    )(trial, resid, energy.reshape(rows // LANES, LANES), shift.reshape(1, new))


def solution(mesh):
    in_specs = (P(("gx", "gy"), None), P(("gx", "gy"), None), P(("gx", "gy")), P())
    out_specs = P(("gx", "gy"), None)
    body = functools.partial(per_device, mesh.shape["gx"], mesh.shape["gy"])
    return jax.shard_map(body, mesh=mesh, in_specs=in_specs, out_specs=out_specs, check_vma=False)
```
